32 devices in a mesh: day: 2 (over x), chan: 16 (over z, y, core).
Axes of the slice: x: 2, y: 2, z: 4, core: 2. Of those that a mesh axis runs over, the one named last changes fastest.
Arguments:
- file_blocks: bfloat16 [224, 16, 1024], P(('day', 'chan')), parts along dimension 0, may hold values from -132 to 132
- block_target: int32 [224], P(('day', 'chan')), parts along dimension 0, may hold values from -1 to 63, as said below
Outputs:
- correlations: bfloat16 [512, 64, 144], P(('day', 'chan')), parts along dimension 0
The draws below stay inside these ranges and needn't reach their ends.
There are 2 independent parts, one for each index of `day`. The reference program is written for one: setup_inputs(seed, part) draws one part's arguments, and reference() takes and returns one part's arrays. A program takes and returns all parts, laid end to end along the dimension named above; each array names one. Nothing has to cross between parts.
Inputs may be any that keep to these rules, and one draw needn't show every extreme that they name: `block_target`: -1 marks an empty slot and a device's filled slots come first; each device holds 1 to 7 blocks. A value v names window v % 4 of channel owner v // 4; every such pair appears exactly once. Devices 2k and 2k+1 together hold exactly the 8 blocks of owners 2k and 2k+1; in every draw some device holds all 4 blocks of its neighbour owner in the pair.
All inputs are finite; a program needn't handle non-finite values.
Results may differ from the reference program's by a relative error of at most 0.0073.
Values may be sent and summed in bfloat16 or wider, within the bound.
A program may use at most 64 MiB of HBM per device.

```python
import math
import jax
import jax.numpy as jnp
from jax import lax

CH_DEV = 16
NW = 4
WIN = 1024
BANDS = 128
BAND_LO = 16
SMOOTH = 4
LAGS = 64
SLOTS = 7
N_CHAN = 16


def pair_layout(key):
    pairs = N_CHAN // 2
    items = 2 * NW
    keys = jax.random.split(jax.random.fold_in(key, 41), 5)
    pair_ids = jnp.arange(pairs, dtype=jnp.int32)
    spread = jax.random.randint(keys[0], (pairs,), 0, NW).astype(jnp.int32)
    forced = jax.random.randint(keys[1], (), 0, pairs).astype(jnp.int32)
    spread = jnp.where(pair_ids == forced, NW - 1, spread)
    flips = jax.random.randint(keys[2], (pairs,), 0, 2).astype(jnp.int32)
    first_count = jnp.where(flips == 1, NW + spread, NW - spread)
    orders = jax.vmap(lambda sub_key: jax.random.permutation(sub_key, items))(jax.random.split(keys[3], pairs)).astype(jnp.int32)
    chosen = (1 - flips) * NW + jax.random.randint(keys[4], (pairs,), 0, NW).astype(jnp.int32)
    spots = jnp.where(flips == 0, 0, items - 1).astype(jnp.int32)

    def adjust(order_row, picked, place):
        found = jnp.argmax(order_row == picked)
        moved = order_row.at[found].set(order_row[place])
        return moved.at[place].set(picked)
    adjusted = jax.vmap(adjust)(orders, chosen, spots)
    orders = jnp.where((pair_ids == forced)[:, None], adjusted, orders)
    slot_ids = jnp.arange(SLOTS, dtype=jnp.int32)
    first_index = jnp.broadcast_to(slot_ids[None, :], (pairs, SLOTS))
    first_valid = slot_ids[None, :] < first_count[:, None]
    second_index = first_count[:, None] + slot_ids[None, :]
    second_valid = slot_ids[None, :] < (items - first_count)[:, None]
    index_all = jnp.stack([first_index, second_index], axis=1)
    valid_all = jnp.stack([first_valid, second_valid], axis=1)
    clipped = jnp.clip(index_all, 0, items - 1).reshape(pairs, 2 * SLOTS)
    picked_items = jnp.take_along_axis(orders, clipped, axis=1).reshape(pairs, 2, SLOTS)
    targets = (2 * pair_ids[:, None, None] + picked_items // NW) * NW + picked_items % NW
    targets = jnp.where(valid_all, targets, -1)
    return targets.reshape(-1).astype(jnp.int32)


def draw_block_target(key, part):
    return pair_layout(key)


def draw_file_blocks(key, part):
    keys = jax.random.split(jax.random.fold_in(key, 23), 5)
    rows = N_CHAN * SLOTS
    scales = jnp.exp(jax.random.uniform(keys[0], (rows, CH_DEV, 1), jnp.float32, 0.0, math.log(10.0)))
    tones = jax.random.randint(keys[1], (rows, CH_DEV, 1), BAND_LO, BAND_LO + BANDS).astype(jnp.int32)
    heights = jax.random.uniform(keys[2], (rows, CH_DEV, 1), jnp.float32, 1.0, 4.0)
    phases = jax.random.uniform(keys[3], (rows, CH_DEV, 1), jnp.float32, -math.pi, math.pi)
    times = jnp.arange(WIN, dtype=jnp.int32)
    angle = 2.0 * math.pi / WIN * (tones * times[None, None, :] % WIN).astype(jnp.float32) + phases
    noise = jnp.clip(jax.random.normal(keys[4], (rows, CH_DEV, WIN), jnp.float32), -5.0, 5.0)
    values = scales * (noise + heights * jnp.sin(angle))
    return values.astype(jnp.bfloat16)


def setup_inputs(seed: int = 0, part: int = 0) -> dict:
    key_of = jax.random.split(jax.random.key(seed), 3)
    part_splits = jax.random.split(jax.random.fold_in(key_of[2], part), 3)
    file_blocks = draw_file_blocks(jax.random.fold_in(jax.random.fold_in(key_of[2], part), 71), part)
    block_target = draw_block_target(jax.random.fold_in(jax.random.fold_in(key_of[2], part), 71), part)
    return {"file_blocks": file_blocks, "block_target": block_target}


def fourier_table(samples, bands, band_low):
    times = jnp.arange(samples, dtype=jnp.int32)
    bins = band_low + jnp.arange(bands, dtype=jnp.int32)
    phase = times[:, None] * bins[None, :] % samples
    angle = 2.0 * math.pi / samples * phase.astype(jnp.float32)
    taper = 0.5 - 0.5 * jnp.cos(2.0 * math.pi / samples * times.astype(jnp.float32))
    rows = jnp.concatenate([taper[:, None] * jnp.cos(angle), -taper[:, None] * jnp.sin(angle)], axis=1)
    return rows.astype(jnp.bfloat16)

def lag_table(samples, bands, band_low, lags, windows):
    bins = band_low + jnp.arange(bands, dtype=jnp.int32)
    delays = jnp.arange(lags, dtype=jnp.int32) - lags // 2
    phase = bins[:, None] * delays[None, :] % samples
    angle = 2.0 * math.pi / samples * phase.astype(jnp.float32)
    weight = 1.0 / math.sqrt(windows * bands)
    rows = jnp.stack([jnp.cos(angle) * weight, -jnp.sin(angle) * weight])
    return rows.astype(jnp.bfloat16)

def whiten(spectra, bands, smooth):
    real_part = spectra[..., :bands]
    imag_part = spectra[..., bands:]
    power = real_part * real_part + imag_part * imag_part
    widths = [(0, 0)] * (power.ndim - 1) + [(smooth, smooth)]
    padded = jnp.pad(power, widths)
    nearby = padded[..., 0:bands]
    for shift_bins in range(1, 2 * smooth + 1):
        nearby = nearby + padded[..., shift_bins:shift_bins + bands]
    level = nearby / (2 * smooth + 1) + 0.25 * lax.optimization_barrier(jnp.mean(power, axis=-1, keepdims=True)) + 1e-05
    factor = 1.0 / jnp.sqrt(level)
    return jnp.concatenate([real_part * factor, imag_part * factor], axis=-1).astype(jnp.bfloat16)

def pair_block(own_block, other_block, lag_rows, bands):
    windows = own_block.shape[0]
    own_wide = own_block.astype(jnp.float32)
    other_wide = other_block.astype(jnp.float32)
    own_split = own_wide.reshape(windows, own_wide.shape[1], 2, bands)
    other_split = other_wide.reshape(windows, other_wide.shape[1], 2, bands)
    same_part = jnp.einsum('wicb,wjcb->bij', own_split, other_split)
    turned = jnp.einsum('wib,wjb->bij', own_split[:, :, 1], other_split[:, :, 0]) - jnp.einsum('wib,wjb->bij', own_split[:, :, 0], other_split[:, :, 1])
    cross = jnp.stack([same_part, turned]).astype(jnp.bfloat16)
    result = jnp.einsum('pbij,pbt->itj', cross.astype(jnp.float32), lag_rows.astype(jnp.float32))
    return result.astype(jnp.bfloat16)

def reference(file_blocks, block_target):
    transform = fourier_table(WIN, BANDS, BAND_LO)
    lag_rows = lag_table(WIN, BANDS, BAND_LO, LAGS, NW)
    total = N_CHAN * NW
    filled = block_target >= 0
    where_to = jnp.where(filled, block_target, total).astype(jnp.int32)
    slot_of = jnp.zeros((total + 1,), jnp.int32).at[where_to].set(jnp.arange(block_target.shape[0], dtype=jnp.int32))
    records = file_blocks[slot_of[:total]]
    records = records.reshape(N_CHAN, NW, CH_DEV, WIN).transpose(1, 0, 2, 3).reshape(NW * N_CHAN * CH_DEV, WIN)
    spectra = jnp.dot(records, transform, preferred_element_type=jnp.float32)
    spectra = spectra.reshape(NW, N_CHAN * CH_DEV, 2 * BANDS)
    whitened = whiten(spectra, BANDS, SMOOTH).reshape(NW, N_CHAN, CH_DEV, 2 * BANDS)
    half_cycle = N_CHAN // 2

    def per_owner(owner_index):
        own_block = lax.dynamic_index_in_dim(whitened, owner_index, 1, keepdims=False)

        def per_offset(offset):
            source = ((owner_index + offset) % N_CHAN).astype(jnp.int32)
            other_block = lax.dynamic_index_in_dim(whitened, source, 1, keepdims=False)
            return pair_block(own_block, other_block, lag_rows, BANDS)
        blocks = jax.vmap(per_offset)(jnp.arange(half_cycle + 1, dtype=jnp.int32))
        return blocks.transpose(1, 2, 0, 3).reshape(CH_DEV, LAGS, (half_cycle + 1) * CH_DEV)
    result = lax.map(per_owner, jnp.arange(N_CHAN, dtype=jnp.int32))
    return result.reshape(N_CHAN * CH_DEV, LAGS, (half_cycle + 1) * CH_DEV)
```

```python
import functools
import math

import jax
import jax.numpy as jnp
import numpy as np
from jax import lax
from jax.experimental import pallas as pl
from jax.experimental.pallas import tpu as pltpu
from jax.sharding import PartitionSpec as P

NW = 4
BANDS = 128
BAND_LO = 16
SMOOTH = 4
LAGS = 64
MESH = pl.DeviceIdType.MESH


def fourier_table(samples, bands, band_low):
    times = np.arange(samples, dtype=np.int32)
    bins = band_low + np.arange(bands, dtype=np.int32)
    phase = times[:, None] * bins[None, :] % samples
    angle = np.float32(2.0 * math.pi / samples) * phase.astype(np.float32)
    turn = np.float32(2.0 * math.pi / samples) * times.astype(np.float32)
    taper = np.float32(0.5) - np.float32(0.5) * np.cos(turn)
    rows = np.concatenate([taper[:, None] * np.cos(angle), -taper[:, None] * np.sin(angle)], axis=1)
    return rows.astype(jnp.bfloat16)


def lag_table(samples, bands, band_low, lags, windows):
    bins = band_low + np.arange(bands, dtype=np.int32)
    delays = np.arange(lags, dtype=np.int32) - lags // 2
    phase = bins[:, None] * delays[None, :] % samples
    angle = np.float32(2.0 * math.pi / samples) * phase.astype(np.float32)
    weight = np.float32(1.0 / math.sqrt(windows * bands))
    rows = np.concatenate([np.cos(angle) * weight, -np.sin(angle) * weight], axis=0)
    return np.ascontiguousarray(rows.T).astype(jnp.bfloat16)


def shifted(values, steps):
    bands = values.shape[1]
    lane = lax.broadcasted_iota(jnp.int32, values.shape, 1)
    moved = pltpu.roll(values, steps % bands, 1)
    inside = lane >= steps if steps > 0 else lane < bands + steps
    return jnp.where(inside, moved, 0.0)


def whiten(spectra):
    real_part = spectra[:, :BANDS]
    imag_part = spectra[:, BANDS:]
    power = real_part * real_part + imag_part * imag_part
    below = power + shifted(power, 1)
    below = shifted(below + shifted(below, 2), 1)
    above = power + shifted(power, -1)
    above = shifted(above + shifted(above, -2), -1)
    nearby = power + below + above
    mean = jnp.sum(power, axis=1, keepdims=True) * (1.0 / BANDS)
    level = nearby * (1.0 / (2 * SMOOTH + 1)) + 0.25 * mean + 1e-05
    factor = lax.rsqrt(level)
    return jnp.concatenate([real_part * factor, imag_part * factor], axis=1).astype(jnp.bfloat16)


def kernel(
    devices, target_ref, files_ref, transform_ref, lag_ref, out_ref,
    canon, incoming, blocks, own, cross,
    swap_send, swap_recv, ring_send, ring_recv, pass_send, pass_recv,
):
    slots, channels, samples = files_ref.shape
    chips = devices // 2
    reach = chips // 2
    half = devices // 2
    me = lax.axis_index("chan")
    chip = me // 2
    core = lax.rem(me, 2)
    partner = 2 * chip + 1 - core

    def same_core(step):
        return 2 * lax.rem(chip + step, chips) + core

    barrier = pltpu.get_barrier_semaphore()
    pl.semaphore_signal(barrier, inc=1, device_id={"chan": partner}, device_id_type=MESH)

    @pl.loop(1, chips)
    def _(step):
        pl.semaphore_signal(barrier, inc=1, device_id={"chan": same_core(step)}, device_id_type=MESH)

    pieces = []
    for item in range(2 * NW):
        value = chip * (2 * NW) + item
        slot = jnp.int32(0)
        found = jnp.int32(0)
        for q in range(slots):
            hit = target_ref[q] == value
            slot = jnp.where(hit, q, slot)
            found = jnp.where(hit, 1, found)
        block = files_ref[slot]
        pieces.append(jnp.where(found > 0, block, jnp.zeros_like(block)))
    records = jnp.concatenate(pieces, axis=0)
    spectra = jnp.dot(records, transform_ref[...], preferred_element_type=jnp.float32)
    canon[...] = whiten(spectra).reshape(canon.shape)

    pl.semaphore_wait(barrier, chips)
    swap = pltpu.make_async_remote_copy(
        src_ref=canon, dst_ref=incoming, send_sem=swap_send, recv_sem=swap_recv,
        device_id={"chan": partner}, device_id_type=MESH,
    )
    swap.start()
    swap.wait()
    blocks[pl.ds(0, 2)] = canon[...] + incoming[...]

    def ring(step):
        return pltpu.make_async_remote_copy(
            src_ref=blocks.at[core], dst_ref=blocks.at[2 * step + core],
            send_sem=ring_send.at[step - 1], recv_sem=ring_recv.at[step - 1],
            device_id={"chan": same_core(chips - step)}, device_id_type=MESH,
        )

    def handed(step):
        return pltpu.make_async_remote_copy(
            src_ref=blocks.at[2 * step + core], dst_ref=blocks.at[2 * step + core],
            send_sem=pass_send.at[step - 1], recv_sem=pass_recv.at[step - 1],
            device_id={"chan": partner}, device_id_type=MESH,
        )

    @pl.loop(0, reach)
    def _(back):
        ring(reach - back).start()

    mine = blocks[core].astype(jnp.float32)
    own[:, 0] = mine[:, :, :BANDS]
    own[:, 1] = mine[:, :, BANDS:]

    def pairs(flat):
        other = blocks[flat].astype(jnp.float32)
        real_other = [other[w, :, :BANDS] for w in range(NW)]
        imag_other = [other[w, :, BANDS:] for w in range(NW)]
        rows = pl.ds(pl.multiple_of((flat - core) * channels, channels), channels)
        for i in range(channels):
            same = None
            for w in range(NW):
                real_own = own[w, 0, pl.ds(i, 1), :]
                imag_own = own[w, 1, pl.ds(i, 1), :]
                s = real_own * real_other[w] + imag_own * imag_other[w]
                t = imag_own * real_other[w] - real_own * imag_other[w]
                same, turned = (s, t) if same is None else (same + s, turned + t)
            cross[i, rows, :] = jnp.concatenate([same, turned], axis=1).astype(jnp.bfloat16)

    pairs(core)

    @pl.when(core == 0)
    def _():
        pairs(1)

    @pl.loop(1, reach + 1)
    def _(step):
        ring(step).wait()
        handed(step).start()
        pairs(2 * step + core)

        @pl.when(step > 1)
        def _():
            handed(step - 1).wait()
            pairs(2 * (step - 1) + 1 - core)

    handed(reach).wait()

    @pl.when(core == 1)
    def _():
        pairs(2 * reach)

    for i in range(channels):
        out_ref[i] = lax.dot_general(
            lag_ref[...], cross[i], (((1,), (1,)), ((), ())), preferred_element_type=jnp.float32
        ).astype(out_ref.dtype)


def shards(file_blocks, block_target):
    slots, channels, samples = file_blocks.shape
    devices = lax.axis_size("chan")
    reach = devices // 4
    columns = (devices // 2 + 1) * channels
    transform = jnp.asarray(fourier_table(samples, BANDS, BAND_LO))
    lag_rows = jnp.asarray(lag_table(samples, BANDS, BAND_LO, LAGS, NW))
    vmem = pl.BlockSpec(memory_space=pltpu.VMEM)
    return pl.pallas_call(
        functools.partial(kernel, devices),
        out_shape=jax.ShapeDtypeStruct((channels, LAGS, columns), jnp.bfloat16),
        in_specs=[pl.BlockSpec(memory_space=pltpu.SMEM), vmem, vmem, vmem],
        out_specs=vmem,
        scratch_shapes=[
            pltpu.VMEM((2, NW, channels, 2 * BANDS), jnp.bfloat16),
            pltpu.VMEM((2, NW, channels, 2 * BANDS), jnp.bfloat16),
            pltpu.VMEM((2 * (reach + 1), NW, channels, 2 * BANDS), jnp.bfloat16),
            pltpu.VMEM((NW, 2, channels, BANDS), jnp.float32),
            pltpu.VMEM((channels, columns, 2 * BANDS), jnp.bfloat16),
            pltpu.SemaphoreType.DMA,
            pltpu.SemaphoreType.DMA,
            pltpu.SemaphoreType.DMA((reach,)),
            pltpu.SemaphoreType.DMA((reach,)),
            pltpu.SemaphoreType.DMA((reach,)),
            pltpu.SemaphoreType.DMA((reach,)),
        ],
        compiler_params=pltpu.CompilerParams(collective_id=0, has_side_effects=True),
        name="correlate",
    )(block_target, file_blocks, transform, lag_rows)


def solution(mesh):
    return jax.shard_map(
        shards,
        mesh=mesh,
        in_specs=(P(("day", "chan"), None, None), P(("day", "chan"))),
        out_specs=P(("day", "chan"), None, None),
        check_vma=False,
    )
```

```python
import functools
import math

import jax
import jax.numpy as jnp
import numpy as np
from jax import lax
from jax.experimental import pallas as pl
from jax.experimental.pallas import tpu as pltpu
from jax.sharding import PartitionSpec as P

NW = 4
BANDS = 128
BAND_LO = 16
SMOOTH = 4
LAGS = 64
MESH = pl.DeviceIdType.MESH


def fourier_table(samples, bands, band_low):
    times = np.arange(samples, dtype=np.int32)
    bins = band_low + np.arange(bands, dtype=np.int32)
    phase = times[:, None] * bins[None, :] % samples
    angle = np.float32(2.0 * math.pi / samples) * phase.astype(np.float32)
    turn = np.float32(2.0 * math.pi / samples) * times.astype(np.float32)
    taper = np.float32(0.5) - np.float32(0.5) * np.cos(turn)
    rows = np.concatenate([taper[:, None] * np.cos(angle), -taper[:, None] * np.sin(angle)], axis=1)
    return rows.astype(jnp.bfloat16)


def lag_table(samples, bands, band_low, lags, windows):
    bins = band_low + np.arange(bands, dtype=np.int32)
    delays = np.arange(lags, dtype=np.int32) - lags // 2
    phase = bins[:, None] * delays[None, :] % samples
    angle = np.float32(2.0 * math.pi / samples) * phase.astype(np.float32)
    weight = np.float32(1.0 / math.sqrt(windows * bands))
    rows = np.concatenate([np.cos(angle) * weight, -np.sin(angle) * weight], axis=0)
    return np.ascontiguousarray(rows.T).astype(jnp.bfloat16)


def shifted(values, steps):
    bands = values.shape[1]
    lane = lax.broadcasted_iota(jnp.int32, values.shape, 1)
    moved = pltpu.roll(values, steps % bands, 1)
    inside = lane >= steps if steps > 0 else lane < bands + steps
    return jnp.where(inside, moved, 0.0)


def whiten(spectra):
    real_part = spectra[:, :BANDS]
    imag_part = spectra[:, BANDS:]
    power = real_part * real_part + imag_part * imag_part
    below = power + shifted(power, 1)
    below = shifted(below + shifted(below, 2), 1)
    above = power + shifted(power, -1)
    above = shifted(above + shifted(above, -2), -1)
    nearby = power + below + above
    mean = jnp.sum(power, axis=1, keepdims=True) * (1.0 / BANDS)
    level = nearby * (1.0 / (2 * SMOOTH + 1)) + 0.25 * mean + 1e-05
    factor = lax.rsqrt(level)
    return jnp.concatenate([real_part * factor, imag_part * factor], axis=1).astype(jnp.bfloat16)


def kernel(
    devices, target_hbm, files_hbm, transform_hbm, lag_hbm, out_ref,
    target_ref, files_ref, transform_ref, lag_ref, canon, incoming, blocks, own, cross,
    load_sems, swap_send, swap_recv, ring_send, ring_recv, pass_send, pass_recv,
):
    slots, channels, samples = files_ref.shape
    chips = devices // 2
    reach = chips // 2
    half = devices // 2
    me = lax.axis_index("chan")
    chip = me // 2
    core = lax.rem(me, 2)
    partner = 2 * chip + 1 - core

    def same_core(step):
        return 2 * lax.rem(chip + step, chips) + core

    barrier = pltpu.get_barrier_semaphore()
    pl.semaphore_signal(barrier, inc=1, device_id={"chan": partner}, device_id_type=MESH)

    @pl.loop(1, chips)
    def _(step):
        pl.semaphore_signal(barrier, inc=1, device_id={"chan": same_core(step)}, device_id_type=MESH)

    loads = [
        pltpu.make_async_copy(source, target, load_sems.at[index])
        for index, (source, target) in enumerate([
            (target_hbm, target_ref), (files_hbm, files_ref),
            (transform_hbm, transform_ref), (lag_hbm, lag_ref),
        ])
    ]
    for load in loads:
        load.start()
    for load in loads:
        load.wait()

    pieces = []
    for item in range(2 * NW):
        value = chip * (2 * NW) + item
        slot = jnp.int32(0)
        found = jnp.int32(0)
        for q in range(slots):
            hit = target_ref[q] == value
            slot = jnp.where(hit, q, slot)
            found = jnp.where(hit, 1, found)
        block = files_ref[slot]
        pieces.append(jnp.where(found > 0, block, jnp.zeros_like(block)))
    records = jnp.concatenate(pieces, axis=0)
    spectra = jnp.dot(records, transform_ref[...], preferred_element_type=jnp.float32)
    canon[...] = whiten(spectra).reshape(canon.shape)

    pl.semaphore_wait(barrier, chips)
    swap = pltpu.make_async_remote_copy(
        src_ref=canon, dst_ref=incoming, send_sem=swap_send, recv_sem=swap_recv,
        device_id={"chan": partner}, device_id_type=MESH,
    )
    swap.start()
    swap.wait()
    blocks[pl.ds(0, 2)] = canon[...] + incoming[...]

    def ring(step):
        return pltpu.make_async_remote_copy(
            src_ref=blocks.at[core], dst_ref=blocks.at[2 * step + core],
            send_sem=ring_send.at[step - 1], recv_sem=ring_recv.at[step - 1],
            device_id={"chan": same_core(chips - step)}, device_id_type=MESH,
        )

    def handed(step):
        return pltpu.make_async_remote_copy(
            src_ref=blocks.at[2 * step + core], dst_ref=blocks.at[2 * step + core],
            send_sem=pass_send.at[step - 1], recv_sem=pass_recv.at[step - 1],
            device_id={"chan": partner}, device_id_type=MESH,
        )

    @pl.loop(0, reach)
    def _(back):
        ring(reach - back).start()

    mine = blocks[core].astype(jnp.float32)
    own[:, 0] = mine[:, :, :BANDS]
    own[:, 1] = mine[:, :, BANDS:]

    def pairs(flat):
        other = blocks[flat].astype(jnp.float32)
        real_other = [other[w, :, :BANDS] for w in range(NW)]
        imag_other = [other[w, :, BANDS:] for w in range(NW)]
        rows = pl.ds(pl.multiple_of((flat - core) * channels, channels), channels)
        for i in range(channels):
            same = None
            for w in range(NW):
                real_own = own[w, 0, pl.ds(i, 1), :]
                imag_own = own[w, 1, pl.ds(i, 1), :]
                s = real_own * real_other[w] + imag_own * imag_other[w]
                t = imag_own * real_other[w] - real_own * imag_other[w]
                same, turned = (s, t) if same is None else (same + s, turned + t)
            cross[i, rows, :] = jnp.concatenate([same, turned], axis=1).astype(jnp.bfloat16)

    pairs(core)

    @pl.when(core == 0)
    def _():
        pairs(1)

    def lagged(first, count):
        for i in range(channels):
            out_ref[i, :, pl.ds(first, count)] = lax.dot_general(
                lag_ref[...], cross[i, pl.ds(first, count), :], (((1,), (1,)), ((), ())),
                preferred_element_type=jnp.float32,
            ).astype(out_ref.dtype)

    def take_handed(step):
        handed(step).wait()
        pairs(2 * step + 1 - core)

    @pl.loop(1, reach)
    def _(step):
        ring(step).wait()
        handed(step).start()
        pairs(2 * step + core)
        pl.when(step > 1)(lambda: take_handed(step - 1))

    take_handed(reach - 1)
    ring(reach).wait()
    handed(reach).start()
    pairs(2 * reach + core)
    lagged(half * channels, channels)
    handed(reach).wait()
    pl.when(core == 1)(lambda: pairs(2 * reach))
    lagged(0, half * channels)


def shards(file_blocks, block_target):
    slots, channels, samples = file_blocks.shape
    devices = lax.axis_size("chan")
    reach = devices // 4
    columns = (devices // 2 + 1) * channels
    transform = jnp.asarray(fourier_table(samples, BANDS, BAND_LO))
    lag_rows = jnp.asarray(lag_table(samples, BANDS, BAND_LO, LAGS, NW))
    hbm = pl.BlockSpec(memory_space=pltpu.HBM)
    vmem_bytes = 2 * columns * channels * 2 * BANDS * 2 + (12 << 20)
    return pl.pallas_call(
        functools.partial(kernel, devices),
        out_shape=jax.ShapeDtypeStruct((channels, LAGS, columns), jnp.bfloat16),
        in_specs=[hbm, hbm, hbm, hbm],
        out_specs=pl.BlockSpec(memory_space=pltpu.VMEM),
        scratch_shapes=[
            pltpu.SMEM(block_target.shape, jnp.int32),
            pltpu.VMEM(file_blocks.shape, jnp.bfloat16),
            pltpu.VMEM(transform.shape, jnp.bfloat16),
            pltpu.VMEM(lag_rows.shape, jnp.bfloat16),
            pltpu.VMEM((2, NW, channels, 2 * BANDS), jnp.bfloat16),
            pltpu.VMEM((2, NW, channels, 2 * BANDS), jnp.bfloat16),
            pltpu.VMEM((2 * (reach + 1), NW, channels, 2 * BANDS), jnp.bfloat16),
            pltpu.VMEM((NW, 2, channels, BANDS), jnp.float32),
            pltpu.VMEM((channels, columns, 2 * BANDS), jnp.bfloat16),
            pltpu.SemaphoreType.DMA((4,)),
            pltpu.SemaphoreType.DMA,
            pltpu.SemaphoreType.DMA,
            pltpu.SemaphoreType.DMA((reach,)),
            pltpu.SemaphoreType.DMA((reach,)),
            pltpu.SemaphoreType.DMA((reach,)),
            pltpu.SemaphoreType.DMA((reach,)),
        ],
        compiler_params=pltpu.CompilerParams(
            collective_id=0, has_side_effects=True, vmem_limit_bytes=vmem_bytes
        ),
        name="correlate",
    )(*[
        pltpu.with_memory_space_constraint(value, pltpu.HBM)
        for value in (block_target, file_blocks, transform, lag_rows)
    ])


def solution(mesh):
    return jax.shard_map(
        shards,
        mesh=mesh,
        in_specs=(P(("day", "chan"), None, None), P(("day", "chan"))),
        out_specs=P(("day", "chan"), None, None),
        check_vma=False,
    )
```

```python
import functools
import math

import jax
import jax.numpy as jnp
import numpy as np
from jax import lax
from jax.experimental import pallas as pl
from jax.experimental.pallas import tpu as pltpu
from jax.sharding import PartitionSpec as P

NW = 4
BANDS = 128
BAND_LO = 16
SMOOTH = 4
LAGS = 64
MESH = pl.DeviceIdType.MESH


def fourier_table(samples, bands, band_low):
    times = np.arange(samples, dtype=np.int32)
    bins = band_low + np.arange(bands, dtype=np.int32)
    phase = times[:, None] * bins[None, :] % samples
    angle = np.float32(2.0 * math.pi / samples) * phase.astype(np.float32)
    turn = np.float32(2.0 * math.pi / samples) * times.astype(np.float32)
    taper = np.float32(0.5) - np.float32(0.5) * np.cos(turn)
    rows = np.concatenate([taper[:, None] * np.cos(angle), -taper[:, None] * np.sin(angle)], axis=1)
    return rows.astype(jnp.bfloat16)


def lag_table(samples, bands, band_low, lags, windows):
    bins = band_low + np.arange(bands, dtype=np.int32)
    delays = np.arange(lags, dtype=np.int32) - lags // 2
    phase = bins[:, None] * delays[None, :] % samples
    angle = np.float32(2.0 * math.pi / samples) * phase.astype(np.float32)
    weight = np.float32(1.0 / math.sqrt(windows * bands))
    rows = np.concatenate([np.cos(angle) * weight, -np.sin(angle) * weight], axis=0)
    return np.ascontiguousarray(rows.T).astype(jnp.bfloat16)


def shifted(values, steps):
    bands = values.shape[1]
    lane = lax.broadcasted_iota(jnp.int32, values.shape, 1)
    moved = pltpu.roll(values, steps % bands, 1)
    inside = lane >= steps if steps > 0 else lane < bands + steps
    return jnp.where(inside, moved, 0.0)


def whiten(spectra):
    real_part = spectra[:, :BANDS]
    imag_part = spectra[:, BANDS:]
    power = real_part * real_part + imag_part * imag_part
    below = power + shifted(power, 1)
    below = shifted(below + shifted(below, 2), 1)
    above = power + shifted(power, -1)
    above = shifted(above + shifted(above, -2), -1)
    nearby = power + below + above
    mean = jnp.sum(power, axis=1, keepdims=True) * (1.0 / BANDS)
    level = nearby * (1.0 / (2 * SMOOTH + 1)) + 0.25 * mean + 1e-05
    factor = lax.rsqrt(level)
    return jnp.concatenate([real_part * factor, imag_part * factor], axis=1).astype(jnp.bfloat16)


def kernel(
    devices, target_hbm, files_hbm, transform_hbm, lag_hbm, out_ref,
    target_ref, files_ref, transform_ref, lag_ref, canon, incoming, blocks, own, cross,
    pair_sem, all_sem, load_sems, swap_send, swap_recv, ring_send, ring_recv, pass_send, pass_recv,
):
    slots, channels, samples = files_ref.shape
    chips = devices // 2
    reach = chips // 2
    half = devices // 2
    me = lax.axis_index("chan")
    chip = me // 2
    core = lax.rem(me, 2)
    partner = 2 * chip + 1 - core

    def same_core(step):
        return 2 * lax.rem(chip + step, chips) + core

    def other_core(step):
        return 2 * lax.rem(chip + step, chips) + 1 - core

    barrier = pltpu.get_barrier_semaphore()

    @pl.when(core == 1)
    def _():
        pl.semaphore_signal(barrier, inc=1, device_id={"chan": partner}, device_id_type=MESH)

    loads = [
        pltpu.make_async_copy(source, target, load_sems.at[index])
        for index, (source, target) in enumerate([
            (target_hbm, target_ref), (files_hbm, files_ref),
            (transform_hbm, transform_ref), (lag_hbm, lag_ref),
        ])
    ]
    for load in loads:
        load.start()

    @pl.when(core == 0)
    def _():
        pl.semaphore_wait(barrier, 1)
        pl.semaphore_signal(pair_sem, inc=1, device_id={"chan": partner}, device_id_type=MESH)

    @pl.when(core == 1)
    def _():
        pl.semaphore_wait(pair_sem, 1)

        @pl.loop(1, chips)
        def _(step):
            pl.semaphore_signal(barrier, inc=1, device_id={"chan": same_core(step)}, device_id_type=MESH)

    for load in loads:
        load.wait()

    pieces = []
    for item in range(2 * NW):
        value = chip * (2 * NW) + item
        slot = jnp.int32(0)
        found = jnp.int32(0)
        for q in range(slots):
            hit = target_ref[q] == value
            slot = jnp.where(hit, q, slot)
            found = jnp.where(hit, 1, found)
        block = files_ref[slot]
        pieces.append(jnp.where(found > 0, block, jnp.zeros_like(block)))
    records = jnp.concatenate(pieces, axis=0)
    spectra = jnp.dot(records, transform_ref[...], preferred_element_type=jnp.float32)
    canon[...] = whiten(spectra).reshape(canon.shape)

    swap = pltpu.make_async_remote_copy(
        src_ref=canon, dst_ref=incoming, send_sem=swap_send, recv_sem=swap_recv,
        device_id={"chan": partner}, device_id_type=MESH,
    )
    swap.start()
    swap.wait()
    blocks[pl.ds(0, 2)] = canon[...] + incoming[...]

    @pl.when(core == 1)
    def _():
        pl.semaphore_wait(barrier, chips - 1)
        pl.semaphore_signal(all_sem, inc=1, device_id={"chan": partner}, device_id_type=MESH)

    @pl.when(core == 0)
    def _():
        pl.semaphore_wait(all_sem, 1)

    def ring(step):
        return pltpu.make_async_remote_copy(
            src_ref=blocks.at[core], dst_ref=blocks.at[2 * step + core],
            send_sem=ring_send.at[step - 1], recv_sem=ring_recv.at[step - 1],
            device_id={"chan": same_core(chips - step)}, device_id_type=MESH,
        )

    def handed(step):
        return pltpu.make_async_remote_copy(
            src_ref=blocks.at[2 * step + core], dst_ref=blocks.at[2 * step + core],
            send_sem=pass_send.at[step - 1], recv_sem=pass_recv.at[step - 1],
            device_id={"chan": partner}, device_id_type=MESH,
        )

    def direct(step):
        return pltpu.make_async_remote_copy(
            src_ref=blocks.at[core], dst_ref=blocks.at[2 * step + core],
            send_sem=pass_send.at[step - 1], recv_sem=pass_recv.at[step - 1],
            device_id={"chan": other_core(chips - step)}, device_id_type=MESH,
        )

    pl.loop(1, reach + 1)(lambda step: ring(step).start())
    pl.when(core == 0)(lambda: direct(reach).start())

    mine = blocks[core].astype(jnp.float32)
    own[:, 0] = mine[:, :, :BANDS]
    own[:, 1] = mine[:, :, BANDS:]

    def pairs(flat):
        other = blocks[flat].astype(jnp.float32)
        real_other = [other[w, :, :BANDS] for w in range(NW)]
        imag_other = [other[w, :, BANDS:] for w in range(NW)]
        rows = pl.ds(pl.multiple_of((flat - core) * channels, channels), channels)
        for i in range(channels):
            same = None
            for w in range(NW):
                real_own = own[w, 0, pl.ds(i, 1), :]
                imag_own = own[w, 1, pl.ds(i, 1), :]
                s = real_own * real_other[w] + imag_own * imag_other[w]
                t = imag_own * real_other[w] - real_own * imag_other[w]
                same, turned = (s, t) if same is None else (same + s, turned + t)
            cross[i, rows, :] = jnp.concatenate([same, turned], axis=1).astype(jnp.bfloat16)

    pairs(core)

    @pl.when(core == 0)
    def _():
        pairs(1)

    def lagged(first, count):
        for i in range(channels):
            out_ref[i, :, pl.ds(first, count)] = lax.dot_general(
                lag_ref[...], cross[i, pl.ds(first, count), :], (((1,), (1,)), ((), ())),
                preferred_element_type=jnp.float32,
            ).astype(out_ref.dtype)

    def take_handed(step):
        handed(step).wait()
        pairs(2 * step + 1 - core)

    @pl.loop(1, reach)
    def _(step):
        ring(step).wait()
        handed(step).start()
        pairs(2 * step + core)
        pl.when(step > 1)(lambda: take_handed(step - 1))

    take_handed(reach - 1)
    lagged(0, (half - 1) * channels)
    ring(reach).wait()
    pairs(2 * reach + core)
    pl.when(core == 0)(lambda: direct(reach).wait_send())

    @pl.when(core == 1)
    def _():
        handed(reach).wait_recv()
        pairs(2 * reach)

    lagged((half - 1) * channels, 2 * channels)


def shards(file_blocks, block_target):
    slots, channels, samples = file_blocks.shape
    devices = lax.axis_size("chan")
    reach = devices // 4
    columns = (devices // 2 + 1) * channels
    transform = jnp.asarray(fourier_table(samples, BANDS, BAND_LO))
    lag_rows = jnp.asarray(lag_table(samples, BANDS, BAND_LO, LAGS, NW))
    hbm = pl.BlockSpec(memory_space=pltpu.HBM)
    vmem_bytes = 2 * columns * channels * 2 * BANDS * 2 + (12 << 20)
    return pl.pallas_call(
        functools.partial(kernel, devices),
        out_shape=jax.ShapeDtypeStruct((channels, LAGS, columns), jnp.bfloat16),
        in_specs=[hbm, hbm, hbm, hbm],
        out_specs=pl.BlockSpec(memory_space=pltpu.VMEM),
        scratch_shapes=[
            pltpu.SMEM(block_target.shape, jnp.int32),
            pltpu.VMEM(file_blocks.shape, jnp.bfloat16),
            pltpu.VMEM(transform.shape, jnp.bfloat16),
            pltpu.VMEM(lag_rows.shape, jnp.bfloat16),
            pltpu.VMEM((2, NW, channels, 2 * BANDS), jnp.bfloat16),
            pltpu.VMEM((2, NW, channels, 2 * BANDS), jnp.bfloat16),
            pltpu.VMEM((2 * (reach + 1), NW, channels, 2 * BANDS), jnp.bfloat16),
            pltpu.VMEM((NW, 2, channels, BANDS), jnp.float32),
            pltpu.VMEM((channels, columns, 2 * BANDS), jnp.bfloat16),
            pltpu.SemaphoreType.REGULAR,
            pltpu.SemaphoreType.REGULAR,
            pltpu.SemaphoreType.DMA((4,)),
            pltpu.SemaphoreType.DMA,
            pltpu.SemaphoreType.DMA,
            pltpu.SemaphoreType.DMA((reach,)),
            pltpu.SemaphoreType.DMA((reach,)),
            pltpu.SemaphoreType.DMA((reach,)),
            pltpu.SemaphoreType.DMA((reach,)),
        ],
        compiler_params=pltpu.CompilerParams(
            collective_id=0, has_side_effects=True, vmem_limit_bytes=vmem_bytes
        ),
        name="correlate",
    )(*[
        pltpu.with_memory_space_constraint(value, pltpu.HBM)
        for value in (block_target, file_blocks, transform, lag_rows)
    ])


def solution(mesh):
    return jax.shard_map(
        shards,
        mesh=mesh,
        in_specs=(P(("day", "chan"), None, None), P(("day", "chan"))),
        out_specs=P(("day", "chan"), None, None),
        check_vma=False,
    )
```
